32 devices in a mesh: lat: 4 (over y, x), lon: 8 (over z, core).
Axes of the slice: x: 2, y: 2, z: 4, core: 2. Of those that a mesh axis runs over, the one named last changes fastest.
Arguments:
- right_side: float32 [8, 768, 1024], P(None, 'lat', 'lon'), may hold values from -16 to 16
- center: float32 [768, 1024], P('lat', 'lon'), may hold values from 3.7 to 5.5
- couplings: float32 [4, 768, 1024], P(None, 'lat', 'lon'), may hold values from 0.15 to 0.45
- land_sea: int32 [768, 1024], P('lat', 'lon'), may hold values 0 or 1
- fold_partner: int32 [1024], replicated, may hold values from 0 to 1023, as said below
Outputs:
- solution: float32 [8, 768, 1024], P(None, 'lat', 'lon')
- residual: float32 [8, 768, 1024], P(None, 'lat', 'lon')
The draws below stay inside these ranges and needn't reach their ends.
Inputs may be any that keep to these rules, and one draw needn't show every extreme that they name: fold_partner[i] = (s - i) mod 1024 for one integer s, so fold_partner[fold_partner[i]] = i.
All inputs are finite; a program needn't handle non-finite values. No bound on the sum of `land_sea` on one device may be relied on, other than what follows from the above.
Results may differ from the reference program's by a relative error of at most 0.0003.
Values sent between devices are 32-bit elements; how exact they have to be, the bound alone decides.
No kernel may reach another device: no remote copies, remote signals or barrier semaphores. Data moves between devices by JAX's collectives and lax.ppermute only.
A program may use at most 64 MiB of HBM per device.

```python
import math
import jax
import jax.numpy as jnp
from jax import lax

MEMBERS = 8
ITERS = 3
NLAT = 768
NLON = 1024


def draw_right_side(key, part):
    first_key = jax.random.fold_in(key, 11)
    row_pos = jnp.arange(NLAT, dtype=jnp.float32) / NLAT
    col_pos = jnp.arange(NLON, dtype=jnp.float32) / NLON
    scale_map = jnp.exp(0.55 * (row_pos[:, None] + col_pos[None, :]))
    base = jnp.clip(jax.random.normal(first_key, (MEMBERS, NLAT, NLON), jnp.float32), -4.0, 4.0)
    values = base * scale_map[None]
    return values.astype(jnp.float32)


def draw_fold_partner(key, part):
    offset = jax.random.randint(jax.random.fold_in(key, 21), (), 0, NLON)
    return ((offset - jnp.arange(NLON, dtype=jnp.int32)) % NLON).astype(jnp.int32)


def touch_ends(values, rng, least, top_value):
    longest = values.shape.index(max(values.shape))
    spots = []
    for shift in (0, 1):
        where = [jax.random.randint(jax.random.fold_in(rng, axis), (), 0, length) for axis, length in enumerate(values.shape)]
        where[longest] = (where[longest] + shift) % values.shape[longest]
        spots.append(tuple(where))
    return values.at[spots[0]].set(least).at[spots[1]].set(top_value)


def block_scale(key, shape, shards, low, top_value):
    def one(axis_at, blocks):
        steps = jax.random.uniform(jax.random.fold_in(jax.random.fold_in(key, 6), axis_at), (blocks,), jnp.float32, low / len(shards), top_value / len(shards))
        return jnp.repeat(jnp.exp(steps), shape[axis_at] // blocks).reshape((-1,) + (1,) * (len(shape) - axis_at - 1))

    loudness = one(*shards[0])
    for cut in shards[1:]:
        loudness = loudness * one(*cut)
    return loudness


def setup_inputs(seed: int = 0) -> dict:
    arg_keys = jax.random.split(jax.random.key(seed), 6)
    return {
        "right_side": draw_right_side(jax.random.fold_in(arg_keys[5], 71), 0),
        "center": jnp.clip(3.7 + 1.8 * jax.random.uniform(arg_keys[1], (NLAT, NLON), jnp.float32) ** block_scale(arg_keys[1], (NLAT, NLON), ((0, 4), (1, 8)), -0.2, 0.2), 3.7, 5.5),
        "couplings": jnp.clip(jnp.exp(math.log(0.45) - 1.0986122 * jax.random.uniform(arg_keys[2], (4, NLAT, NLON), jnp.float32) ** block_scale(arg_keys[2], (4, NLAT, NLON), ((1, 4), (2, 8)), -0.2, 0.2)), 0.15, 0.45),
        "land_sea": touch_ends((jax.random.randint(arg_keys[3], (NLAT, NLON), 0, 5) < 4).astype(jnp.int32), jax.random.fold_in(arg_keys[3], 1), 0, 1),
        "fold_partner": draw_fold_partner(jax.random.fold_in(arg_keys[5], 71), 0),
    }


def below(values):
    return jnp.concatenate([jnp.zeros_like(values[:1]), values[:-1]], axis=0)


def reference(right_side, center, couplings, land_sea, fold_partner):
    ocean_mask = land_sea.astype(jnp.float32)
    east_coeff = couplings[0]
    north_top = couplings[1][-1]
    fold_coeff = 0.5 * (north_top + north_top[fold_partner])
    top_rows = (jnp.arange(NLAT) == NLAT - 1)[:, None]
    north_coeff = jnp.where(top_rows, fold_coeff[None, :], couplings[1])
    northeast = jnp.where(top_rows, 0.0, couplings[2])
    northwest = jnp.where(top_rows, 0.0, couplings[3])
    west_coeff = jnp.roll(east_coeff, 1, axis=1)
    south_coeff = below(north_coeff)
    southwest = jnp.roll(below(northeast), 1, axis=1)
    southeast = jnp.roll(below(northwest), -1, axis=1)

    def operate(vector):
        fold_ghost = vector[-1][fold_partner]
        upper = jnp.concatenate([vector[1:], fold_ghost[None, :]], axis=0)
        lower = below(vector)
        beside = east_coeff * jnp.roll(vector, -1, axis=1) + west_coeff * jnp.roll(vector, 1, axis=1)
        beside = beside + north_coeff * upper + south_coeff * lower
        beside = beside + northeast * jnp.roll(upper, -1, axis=1) + southwest * jnp.roll(lower, 1, axis=1)
        beside = beside + northwest * jnp.roll(upper, 1, axis=1) + southeast * jnp.roll(lower, -1, axis=1)
        return ocean_mask * (center * vector - beside)

    def solve_one(member_rhs):
        residual = ocean_mask * member_rhs
        solution = jnp.zeros_like(residual)
        scaled = residual / center
        direction = scaled
        gamma_now = jnp.sum(residual * scaled)
        for iteration in range(ITERS):
            image = operate(direction)
            step_size = gamma_now / jnp.sum(direction * image)
            solution = solution + step_size * direction
            residual = residual - step_size * image
            scaled = residual / center
            gamma_next = jnp.sum(residual * scaled)
            direction = scaled + (gamma_next / gamma_now) * direction
            gamma_now = gamma_next
        return solution, residual

    solution, residual = lax.map(solve_one, right_side)
    return solution, residual
```

```python
import jax
import jax.numpy as jnp
from jax import lax
from jax.experimental import pallas as pl
from jax.experimental.pallas import tpu as pltpu
from jax.sharding import PartitionSpec as P

ITERS = 3
DEPTH = ITERS
SUB = 8
TOP = 2 * SUB


def pack_kernel(rhs, center, couplings, land, east, west, north, south):
    members = rhs.shape[0]
    fields = members + couplings.shape[0] + 1
    rows, cols = center.shape
    lane = lax.broadcasted_iota(jnp.int32, (SUB, cols), 1)
    group = 2 * DEPTH

    def chunk_fields(at):
        weight = land[pl.ds(at, SUB), :].astype(jnp.float32) / center[pl.ds(at, SUB), :]
        out = [rhs[m, pl.ds(at, SUB), :] * weight for m in range(members)]
        out += [couplings[c, pl.ds(at, SUB), :] for c in range(couplings.shape[0])]
        return out + [weight]

    def step(index, carry):
        at = pl.multiple_of(index * SUB, SUB)
        values = chunk_fields(at)
        to_east = jnp.zeros((SUB, cols), jnp.float32)
        to_west = jnp.zeros((SUB, cols), jnp.float32)
        for f, value in enumerate(values):
            base = group * f
            moved = pltpu.roll(value, (base + DEPTH) % cols, 1)
            pick_east = jnp.logical_and(lane >= base, lane < base + DEPTH)
            pick_west = jnp.logical_and(lane >= base + DEPTH, lane < base + group)
            to_east = jnp.where(pick_east, moved, to_east)
            to_west = jnp.where(pick_west, moved, to_west)
        east[pl.ds(at, SUB), :] = to_east
        west[pl.ds(at, SUB), :] = to_west
        return carry

    lax.fori_loop(0, rows // SUB, step, 0)
    for ref, at, first in ((north, rows - SUB, SUB - DEPTH), (south, 0, 0)):
        for f, value in enumerate(chunk_fields(at)):
            ref[DEPTH * f : DEPTH * (f + 1), :] = value[first : first + DEPTH, :]
        used = DEPTH * fields
        ref[used:, :] = jnp.zeros((ref.shape[0] - used, cols), jnp.float32)


def stencil_kernel(
    partner, rhs, center, couplings, land, from_west, from_east, from_north, from_south, ring,
    first, second, third, moments, held, coeff, level_one, level_two,
):
    members = rhs.shape[0]
    edges = couplings.shape[0]
    fields = members + edges + 1
    rows, cols = center.shape
    group = 2 * DEPTH
    wide = 2 * cols
    blocks = ring.shape[0]
    packed = ring.shape[1]
    f_east, f_north, f_ne, f_nw, f_weight = (members + c for c in range(5))
    lat_last = lax.axis_index("lat") == lax.axis_size("lat") - 1
    first_col = lax.axis_index("lon") * cols
    lane = lax.broadcasted_iota(jnp.int32, (SUB, cols), 1)
    in_west = lane % group < DEPTH
    bottom = TOP + rows

    zeros = jnp.zeros((SUB, wide), jnp.float32)
    for at in (0, SUB, bottom, bottom + SUB):
        for f in range(fields):
            held[f, at : at + SUB, :] = zeros
    for at in (0, bottom + SUB):
        for m in range(members):
            level_one[m, at : at + SUB, :] = zeros
            level_two[m, at : at + SUB, :] = zeros

    def spread(value, f):
        return pltpu.roll(value, (cols - group * f - DEPTH) % cols, 1)

    def fill(index, carry):
        at = pl.multiple_of(index * SUB, SUB)
        to = pl.multiple_of(index * SUB + TOP, SUB)
        weight = land[pl.ds(at, SUB), :].astype(jnp.float32) / center[pl.ds(at, SUB), :]
        side = jnp.where(in_west, from_west[pl.ds(at, SUB), :], from_east[pl.ds(at, SUB), :])
        for f in range(fields):
            if f < members:
                value = rhs[f, pl.ds(at, SUB), :] * weight
            elif f < f_weight:
                value = couplings[f - members, pl.ds(at, SUB), :]
            else:
                value = weight
            held[f, pl.ds(to, SUB), :cols] = value
            held[f, pl.ds(to, SUB), cols:] = spread(side, f)
        return carry

    lax.fori_loop(0, rows // SUB, fill, 0)

    side_south = from_south[packed : packed + SUB, :]
    for f in range(fields):
        held[f, TOP - DEPTH : TOP, :cols] = from_south[DEPTH * f : DEPTH * (f + 1), :]
        held[f, TOP - DEPTH : TOP, cols:] = spread(side_south, f)[SUB - DEPTH :, :]

    @pl.when(jnp.logical_not(lat_last))
    def _():
        side_north = from_north[packed : packed + SUB, :]
        for f in range(fields):
            held[f, bottom : bottom + DEPTH, :cols] = from_north[DEPTH * f : DEPTH * (f + 1), :]
            held[f, bottom : bottom + DEPTH, cols:] = spread(side_north, f)[:DEPTH, :]

    @pl.when(lat_last)
    def _():
        total = blocks * cols
        shift = cols.bit_length() - 1
        row = lax.broadcasted_iota(jnp.int32, (packed, cols), 0)
        spot = lax.broadcasted_iota(jnp.int32, (packed, cols), 1)

        def of(f):
            return jnp.logical_and(row >= DEPTH * f, row < DEPTH * (f + 1))

        offset = jnp.where(jnp.logical_or(of(f_east), of(f_ne)), -1, jnp.where(of(f_nw), 1, 0))
        beside = jnp.where(spot < cols // 2, spot + cols, spot - cols)
        mirrored = []
        for column in (spot, beside):
            source = partner[0] - first_col + offset - column
            source = jnp.where(source < 0, source + total, source)
            source = jnp.where(source < 0, source + total, source)
            source = jnp.where(source >= total, source - total, source)
            block = lax.shift_right_logical(source, shift)
            place = jnp.bitwise_and(source, cols - 1)
            found = jnp.zeros((packed, cols), jnp.float32)
            for b in range(blocks):
                taken = jnp.take_along_axis(ring[b], place, axis=1, mode="promise_in_bounds")
                found = jnp.where(block == b, taken, found)
            mirrored.append(found)
        for half, found in enumerate(mirrored):
            lanes = slice(half * cols, (half + 1) * cols)
            for f in range(fields):
                back = 2 if f in (f_north, f_ne, f_nw) else 1
                for k in range(DEPTH):
                    at = DEPTH - back - k
                    if at >= 0:
                        spot_row = DEPTH * f + at
                        held[f, bottom + k : bottom + k + 1, lanes] = found[spot_row : spot_row + 1, :]
            top = slice(bottom - 1, bottom)
            across = found[DEPTH * f_north + DEPTH - 1 : DEPTH * (f_north + 1), :]
            held[f_north, top, lanes] = 0.5 * (held[f_north, top, lanes] + across)
            held[f_ne, top, lanes] = jnp.zeros((1, cols), jnp.float32)
            held[f_nw, top, lanes] = jnp.zeros((1, cols), jnp.float32)

    def east_of(value):
        return pltpu.roll(value, wide - 1, 1)

    def west_of(value):
        return pltpu.roll(value, 1, 1)

    def around(ref, at):
        return ref.at[:, pl.ds(pl.multiple_of(at - SUB, SUB), 3 * SUB), :]

    def make_coeff(index, carry):
        at = pl.multiple_of(index * SUB, SUB)
        here = pl.ds(at, SUB)
        near = around(held, at)
        weight = held[f_weight, here, :]
        weight_east = east_of(weight)
        weight_west = west_of(weight)
        coeff[0, here, :] = west_of(weight * held[f_east, here, :])
        coeff[1, here, :] = west_of(weight * held[f_ne, here, :])
        coeff[2, here, :] = weight_west * near[f_nw, SUB - 1 : 2 * SUB - 1, :]
        coeff[3, here, :] = weight_east * held[f_east, here, :]
        coeff[4, here, :] = east_of(weight * held[f_nw, here, :])
        coeff[5, here, :] = weight_east * near[f_ne, SUB - 1 : 2 * SUB - 1, :]
        coeff[6, here, :] = weight * held[f_north, here, :]
        coeff[7, here, :] = weight * near[f_north, SUB - 1 : 2 * SUB - 1, :]
        return carry

    chunks = rows // SUB
    lax.fori_loop(1, chunks + 3, make_coeff, 0)

    def level(source, target, result):
        def chunk(index, carry, inside):
            at = pl.multiple_of(index * SUB, SUB)
            here = pl.ds(at, SUB)
            c = [coeff[k, here, :] for k in range(8)]
            if inside:
                inner = pl.ds(pl.multiple_of(at - TOP, SUB), SUB)
                scale = center[inner, :]
            sums = []
            near = around(source, at)
            for m in range(members):
                mid = source[m, here, :]
                up = near[m, SUB + 1 : 2 * SUB + 1, :]
                down = near[m, SUB - 1 : 2 * SUB - 1, :]
                new = c[6] * up + c[7] * down
                new = new + east_of(c[0] * mid + c[1] * up + c[2] * down)
                new = new + west_of(c[3] * mid + c[4] * up + c[5] * down)
                if target is not None:
                    target[m, here, :] = new
                if inside:
                    kept = new[:, :cols]
                    result[m, inner, :] = kept
                    scaled = scale * mid[:, :cols]
                    sums.append(carry[2 * m] + scaled * mid[:, :cols])
                    sums.append(carry[2 * m + 1] + scaled * kept)
            return tuple(sums) if inside else carry

        start = tuple(jnp.zeros((SUB, cols), jnp.float32) for _ in range(2 * members))
        if target is not None:
            chunk(1, 0, False)
        out = lax.fori_loop(2, chunks + 2, lambda i, s: chunk(i, s, True), start)
        if target is not None:
            chunk(chunks + 2, 0, False)
        return out

    totals = [level(held, level_one, first), level(level_one, level_two, second), level(level_two, None, third)]
    out_row = lax.broadcasted_iota(jnp.int32, (SUB, cols), 0)
    tile = jnp.zeros((SUB, cols), jnp.float32)
    for k in range(2 * DEPTH):
        gathered = jnp.zeros((SUB, cols), jnp.float32)
        for m in range(members):
            one = jnp.sum(totals[k // 2][2 * m + k % 2], axis=0, keepdims=True)
            gathered = jnp.where(out_row == m, one, gathered)
        tile = jnp.where(lane == k, jnp.sum(gathered, axis=1, keepdims=True), tile)
    moments[...] = tile


def combine_kernel(moments, rhs, center, land, first, second, third, solution, residual):
    def inner(p, q):
        total = 0.0
        for i, a in enumerate(p):
            for j, b in enumerate(q):
                total = total + a * b * nu[i + j]
        return total

    nu = [moments[:, k : k + 1] for k in range(2 * DEPTH)]
    one = jnp.ones_like(nu[0])
    scaled = [one]
    direction = [one]
    answer = [jnp.zeros_like(one)] * DEPTH
    gamma = nu[0]
    for iteration in range(DEPTH):
        image = [d - e for d, e in zip(direction + [0.0], [0.0] + direction)]
        step = gamma / inner(direction, image)
        for i, d in enumerate(direction):
            answer[i] = answer[i] + step * d
        scaled = [z - step * q for z, q in zip(scaled + [0.0], image)]
        if iteration + 1 < DEPTH:
            gamma_next = inner(scaled, scaled)
            ratio = gamma_next / gamma
            direction = [z + ratio * d for z, d in zip(scaled, direction + [0.0])]
            gamma = gamma_next

    rows, cols = center.shape
    members = rhs.shape[0]
    wide_answer = [jnp.broadcast_to(a, (members, cols)) for a in answer]
    wide_scaled = [jnp.broadcast_to(a, (members, cols)) for a in scaled]

    def chunk(index, carry):
        here = pl.ds(pl.multiple_of(index * SUB, SUB), SUB)
        scale = center[here, :]
        weight = land[here, :].astype(jnp.float32) / scale
        for m in range(members):
            basis = [rhs[m, here, :] * weight, first[m, here, :], second[m, here, :], third[m, here, :]]
            got = sum(a[m : m + 1, :] * v for a, v in zip(wide_answer, basis))
            left = sum(a[m : m + 1, :] * v for a, v in zip(wide_scaled, basis))
            solution[m, here, :] = got
            residual[m, here, :] = scale * left
        return carry

    lax.fori_loop(0, rows // SUB, chunk, 0)


def shifted(value, axis, by, closed):
    count = lax.axis_size(axis)
    pairs = [(i, (i + by) % count) for i in range(count) if closed or 0 <= i + by < count]
    return lax.ppermute(value, axis, pairs)


def body(right_side, center, couplings, land_sea, fold_partner):
    members, rows, cols = right_side.shape
    fields = members + couplings.shape[0] + 1
    packed = -(-DEPTH * fields // SUB) * SUB
    f32 = jnp.float32
    vmem = pl.BlockSpec(memory_space=pltpu.VMEM)
    smem = pl.BlockSpec(memory_space=pltpu.SMEM)
    params = pltpu.CompilerParams(vmem_limit_bytes=32 * 1024 * 1024)

    def shape(*dims):
        return jax.ShapeDtypeStruct(dims, f32)

    east, west, north, south = pl.pallas_call(
        pack_kernel,
        in_specs=[vmem] * 4,
        out_specs=[vmem] * 4,
        out_shape=[shape(rows, cols), shape(rows, cols), shape(packed, cols), shape(packed, cols)],
        compiler_params=params,
        name="pack",
    )(right_side, center, couplings, land_sea)

    from_west = shifted(east, "lon", 1, True)
    from_east = shifted(west, "lon", -1, True)
    ring = lax.all_gather(north, "lon", axis=0, tiled=False)
    in_west = (lax.broadcasted_iota(jnp.int32, (SUB, cols), 1) % (2 * DEPTH)) < DEPTH
    upper = jnp.where(in_west, from_west[rows - SUB :], from_east[rows - SUB :])
    lower = jnp.where(in_west, from_west[:SUB], from_east[:SUB])
    from_south = shifted(jnp.concatenate([north, upper]), "lat", 1, False)
    from_north = shifted(jnp.concatenate([south, lower]), "lat", -1, False)

    tall = rows + 2 * TOP
    first, second, third, moments = pl.pallas_call(
        stencil_kernel,
        in_specs=[smem] + [vmem] * 9,
        out_specs=[vmem] * 4,
        out_shape=[shape(members, rows, cols)] * 3 + [shape(SUB, cols)],
        scratch_shapes=[
            pltpu.VMEM((fields, tall, 2 * cols), f32),
            pltpu.VMEM((8, tall, 2 * cols), f32),
            pltpu.VMEM((members, tall, 2 * cols), f32),
            pltpu.VMEM((members, tall, 2 * cols), f32),
        ],
        compiler_params=params,
        name="stencil",
    )(fold_partner, right_side, center, couplings, land_sea, from_west, from_east, from_north, from_south, ring)

    for axis in ("lon", "lat"):
        count = lax.axis_size(axis)
        span = 1
        while span < count:
            moments = moments + lax.ppermute(moments, axis, [(i, i ^ span) for i in range(count)])
            span *= 2

    return tuple(
        pl.pallas_call(
            combine_kernel,
            in_specs=[vmem] * 7,
            out_specs=[vmem] * 2,
            out_shape=[shape(members, rows, cols)] * 2,
            compiler_params=params,
            name="combine",
        )(moments, right_side, center, land_sea, first, second, third)
    )


def solution(mesh):
    return jax.shard_map(
        body,
        mesh=mesh,
        in_specs=(
            P(None, "lat", "lon"),
            P("lat", "lon"),
            P(None, "lat", "lon"),
            P("lat", "lon"),
            P(),
        ),
        out_specs=(P(None, "lat", "lon"), P(None, "lat", "lon")),
        check_vma=False,
    )
```

```python
import jax
import jax.numpy as jnp
from jax import lax
from jax.experimental import pallas as pl
from jax.experimental.pallas import tpu as pltpu
from jax.sharding import PartitionSpec as P

ITERS = 3
DEPTH = ITERS
SUB = 8
TOP = 2 * SUB


def pack_kernel(
    rhs, center, couplings, land, east, west, north, south, scaled, weights, edges, scale, mask, arrivals
):
    members = rhs.shape[0]
    fields = members + couplings.shape[0] + 1
    rows, cols = center.shape
    lane = lax.broadcasted_iota(jnp.int32, (SUB, cols), 1)
    group = 2 * DEPTH
    pairs = ((land, mask), (center, scale), (rhs, scaled), (couplings, edges))
    copies = [pltpu.make_async_copy(a, b, arrivals.at[i]) for i, (a, b) in enumerate(pairs)]
    for copy in copies:
        copy.start()
    for copy in copies:
        copy.wait()

    def step(index, carry):
        at = pl.multiple_of(index * SUB, SUB)
        here = pl.ds(at, SUB)
        weight = mask[here, :].astype(jnp.float32) / scale[here, :]
        weights[here, :] = weight
        values = []
        for m in range(members):
            value = scaled[m, here, :] * weight
            scaled[m, here, :] = value
            values.append(value)
        values += [edges[c, here, :] for c in range(edges.shape[0])]
        values.append(weight)
        to_east = jnp.zeros((SUB, cols), jnp.float32)
        to_west = jnp.zeros((SUB, cols), jnp.float32)
        for f, value in enumerate(values):
            base = group * f
            moved = pltpu.roll(value, (base + DEPTH) % cols, 1)
            pick_east = jnp.logical_and(lane >= base, lane < base + DEPTH)
            pick_west = jnp.logical_and(lane >= base + DEPTH, lane < base + group)
            to_east = jnp.where(pick_east, moved, to_east)
            to_west = jnp.where(pick_west, moved, to_west)
        east[here, :] = to_east
        west[here, :] = to_west
        return carry

    lax.fori_loop(0, rows // SUB, step, 0, unroll=2)
    for ref, at in ((north, rows - DEPTH), (south, 0)):
        span = slice(at, at + DEPTH)
        for f in range(fields):
            if f < members:
                value = scaled[f, span, :]
            elif f < fields - 1:
                value = edges[f - members, span, :]
            else:
                value = weights[span, :]
            ref[DEPTH * f : DEPTH * (f + 1), :] = value
        used = DEPTH * fields
        ref[used:, :] = jnp.zeros((ref.shape[0] - used, cols), jnp.float32)


def stencil_kernel(
    partner, scaled, weights, couplings, center, from_west, from_east, from_north, from_south, *rest
):
    *ring, first, second, third, moments, held, coeff, level_one, level_two = rest
    members = scaled.shape[0]
    edges = couplings.shape[0]
    fields = members + edges + 1
    rows, cols = center.shape
    group = 2 * DEPTH
    wide = 2 * cols
    blocks = len(ring)
    packed = ring[0].shape[0]
    f_east, f_north, f_ne, f_nw, f_weight = (members + c for c in range(5))
    lat_last = lax.axis_index("lat") == lax.axis_size("lat") - 1
    first_col = lax.axis_index("lon") * cols
    lane = lax.broadcasted_iota(jnp.int32, (SUB, cols), 1)
    in_west = lane % group < DEPTH
    bottom = TOP + rows

    zeros = jnp.zeros((SUB, wide), jnp.float32)
    for at in (0, SUB, bottom, bottom + SUB):
        for f in range(fields):
            held[f, at : at + SUB, :] = zeros
    for at in (0, bottom + SUB):
        for m in range(members):
            level_one[m, at : at + SUB, :] = zeros
            level_two[m, at : at + SUB, :] = zeros

    def spread(value, f):
        return pltpu.roll(value, (cols - group * f - DEPTH) % cols, 1)

    def fill(index, carry):
        at = pl.multiple_of(index * SUB, SUB)
        to = pl.multiple_of(index * SUB + TOP, SUB)
        side = jnp.where(in_west, from_west[pl.ds(at, SUB), :], from_east[pl.ds(at, SUB), :])
        for f in range(fields):
            if f < members:
                value = scaled[f, pl.ds(at, SUB), :]
            elif f < f_weight:
                value = couplings[f - members, pl.ds(at, SUB), :]
            else:
                value = weights[pl.ds(at, SUB), :]
            held[f, pl.ds(to, SUB), :cols] = value
            held[f, pl.ds(to, SUB), cols:] = spread(side, f)
        return carry

    lax.fori_loop(0, rows // SUB, fill, 0)

    side_south = from_south[packed : packed + SUB, :]
    for f in range(fields):
        held[f, TOP - DEPTH : TOP, :cols] = from_south[DEPTH * f : DEPTH * (f + 1), :]
        held[f, TOP - DEPTH : TOP, cols:] = spread(side_south, f)[SUB - DEPTH :, :]

    @pl.when(jnp.logical_not(lat_last))
    def _():
        side_north = from_north[packed : packed + SUB, :]
        for f in range(fields):
            held[f, bottom : bottom + DEPTH, :cols] = from_north[DEPTH * f : DEPTH * (f + 1), :]
            held[f, bottom : bottom + DEPTH, cols:] = spread(side_north, f)[:DEPTH, :]

    @pl.when(lat_last)
    def _():
        total = blocks * cols
        shift = cols.bit_length() - 1
        row = lax.broadcasted_iota(jnp.int32, (packed, cols), 0)
        spot = lax.broadcasted_iota(jnp.int32, (packed, cols), 1)

        def of(f):
            return jnp.logical_and(row >= DEPTH * f, row < DEPTH * (f + 1))

        offset = jnp.where(jnp.logical_or(of(f_east), of(f_ne)), -1, jnp.where(of(f_nw), 1, 0))
        beside = jnp.where(spot < cols // 2, spot + cols, spot - cols)
        mirrored = []
        for column in (spot, beside):
            source = partner[0] - first_col + offset - column
            source = jnp.where(source < 0, source + total, source)
            source = jnp.where(source < 0, source + total, source)
            source = jnp.where(source >= total, source - total, source)
            block = lax.shift_right_logical(source, shift)
            place = jnp.bitwise_and(source, cols - 1)
            found = jnp.zeros((packed, cols), jnp.float32)
            for b in range(blocks):
                origin = lax.axis_index("lon") - b
                origin = jnp.where(origin < 0, origin + blocks, origin)
                taken = jnp.take_along_axis(ring[b][...], place, axis=1, mode="promise_in_bounds")
                found = jnp.where(block == origin, taken, found)
            mirrored.append(found)
        for half, found in enumerate(mirrored):
            lanes = slice(half * cols, (half + 1) * cols)
            for f in range(fields):
                back = 2 if f in (f_north, f_ne, f_nw) else 1
                for k in range(DEPTH):
                    at = DEPTH - back - k
                    if at >= 0:
                        spot_row = DEPTH * f + at
                        held[f, bottom + k : bottom + k + 1, lanes] = found[spot_row : spot_row + 1, :]
            top = slice(bottom - 1, bottom)
            across = found[DEPTH * f_north + DEPTH - 1 : DEPTH * (f_north + 1), :]
            held[f_north, top, lanes] = 0.5 * (held[f_north, top, lanes] + across)
            held[f_ne, top, lanes] = jnp.zeros((1, cols), jnp.float32)
            held[f_nw, top, lanes] = jnp.zeros((1, cols), jnp.float32)

    def east_of(value):
        return pltpu.roll(value, wide - 1, 1)

    def west_of(value):
        return pltpu.roll(value, 1, 1)

    def around(ref, at):
        return ref.at[:, pl.ds(pl.multiple_of(at - SUB, SUB), 3 * SUB), :]

    def make_coeff(index, carry):
        at = pl.multiple_of(index * SUB, SUB)
        here = pl.ds(at, SUB)
        near = around(held, at)
        weight = held[f_weight, here, :]
        weight_east = east_of(weight)
        weight_west = west_of(weight)
        coeff[0, here, :] = west_of(weight * held[f_east, here, :])
        coeff[1, here, :] = west_of(weight * held[f_ne, here, :])
        coeff[2, here, :] = weight_west * near[f_nw, SUB - 1 : 2 * SUB - 1, :]
        coeff[3, here, :] = weight_east * held[f_east, here, :]
        coeff[4, here, :] = east_of(weight * held[f_nw, here, :])
        coeff[5, here, :] = weight_east * near[f_ne, SUB - 1 : 2 * SUB - 1, :]
        coeff[6, here, :] = weight * held[f_north, here, :]
        coeff[7, here, :] = weight * near[f_north, SUB - 1 : 2 * SUB - 1, :]
        return carry

    chunks = rows // SUB
    lax.fori_loop(1, chunks + 3, make_coeff, 0)

    def level(source, target, result):
        def chunk(index, carry, inside):
            at = pl.multiple_of(index * SUB, SUB)
            here = pl.ds(at, SUB)
            c = [coeff[k, here, :] for k in range(8)]
            if inside:
                inner = pl.ds(pl.multiple_of(at - TOP, SUB), SUB)
                scale = center[inner, :]
            sums = []
            near = around(source, at)
            for m in range(members):
                mid = source[m, here, :]
                up = near[m, SUB + 1 : 2 * SUB + 1, :]
                down = near[m, SUB - 1 : 2 * SUB - 1, :]
                new = c[6] * up + c[7] * down
                new = new + east_of(c[0] * mid + c[1] * up + c[2] * down)
                new = new + west_of(c[3] * mid + c[4] * up + c[5] * down)
                if target is not None:
                    target[m, here, :] = new
                if inside:
                    kept = new[:, :cols]
                    result[m, inner, :] = kept
                    scaled = scale * mid[:, :cols]
                    sums.append(carry[2 * m] + scaled * mid[:, :cols])
                    sums.append(carry[2 * m + 1] + scaled * kept)
            return tuple(sums) if inside else carry

        start = tuple(jnp.zeros((SUB, cols), jnp.float32) for _ in range(2 * members))
        if target is not None:
            chunk(1, 0, False)
        out = lax.fori_loop(2, chunks + 2, lambda i, s: chunk(i, s, True), start)
        if target is not None:
            chunk(chunks + 2, 0, False)
        return out

    totals = [level(held, level_one, first), level(level_one, level_two, second), level(level_two, None, third)]
    out_row = lax.broadcasted_iota(jnp.int32, (SUB, cols), 0)
    tile = jnp.zeros((SUB, cols), jnp.float32)
    for k in range(2 * DEPTH):
        gathered = jnp.zeros((SUB, cols), jnp.float32)
        for m in range(members):
            one = jnp.sum(totals[k // 2][2 * m + k % 2], axis=0, keepdims=True)
            gathered = jnp.where(out_row == m, one, gathered)
        tile = jnp.where(lane == k, jnp.sum(gathered, axis=1, keepdims=True), tile)
    moments[...] = tile


def combine_kernel(moments, zeroth, center, first, second, third, solution, residual):
    def inner(p, q):
        total = 0.0
        for i, a in enumerate(p):
            for j, b in enumerate(q):
                total = total + a * b * nu[i + j]
        return total

    nu = [moments[:, k : k + 1] for k in range(2 * DEPTH)]
    one = jnp.ones_like(nu[0])
    scaled = [one]
    direction = [one]
    answer = [jnp.zeros_like(one)] * DEPTH
    gamma = nu[0]
    for iteration in range(DEPTH):
        image = [d - e for d, e in zip(direction + [0.0], [0.0] + direction)]
        step = gamma / inner(direction, image)
        for i, d in enumerate(direction):
            answer[i] = answer[i] + step * d
        scaled = [z - step * q for z, q in zip(scaled + [0.0], image)]
        if iteration + 1 < DEPTH:
            gamma_next = inner(scaled, scaled)
            ratio = gamma_next / gamma
            direction = [z + ratio * d for z, d in zip(scaled, direction + [0.0])]
            gamma = gamma_next

    rows, cols = center.shape
    members = zeroth.shape[0]
    wide_answer = [jnp.broadcast_to(a, (members, cols)) for a in answer]
    wide_scaled = [jnp.broadcast_to(a, (members, cols)) for a in scaled]

    def chunk(index, carry):
        here = pl.ds(pl.multiple_of(index * SUB, SUB), SUB)
        scale = center[here, :]
        for m in range(members):
            basis = [zeroth[m, here, :], first[m, here, :], second[m, here, :], third[m, here, :]]
            got = sum(a[m : m + 1, :] * v for a, v in zip(wide_answer, basis))
            left = sum(a[m : m + 1, :] * v for a, v in zip(wide_scaled, basis))
            solution[m, here, :] = got
            residual[m, here, :] = scale * left
        return carry

    lax.fori_loop(0, rows // SUB, chunk, 0)


def shifted(value, axis, by, closed):
    count = lax.axis_size(axis)
    pairs = [(i, (i + by) % count) for i in range(count) if closed or 0 <= i + by < count]
    return lax.ppermute(value, axis, pairs)


def body(right_side, center, couplings, land_sea, fold_partner):
    members, rows, cols = right_side.shape
    fields = members + couplings.shape[0] + 1
    packed = -(-DEPTH * fields // SUB) * SUB
    f32 = jnp.float32
    vmem = pl.BlockSpec(memory_space=pltpu.VMEM)
    smem = pl.BlockSpec(memory_space=pltpu.SMEM)
    params = pltpu.CompilerParams(vmem_limit_bytes=32 * 1024 * 1024)

    def shape(*dims):
        return jax.ShapeDtypeStruct(dims, f32)

    east, west, north, south, scaled, weights, edges, scale = pl.pallas_call(
        pack_kernel,
        in_specs=[pl.BlockSpec(memory_space=pl.ANY)] * 4,
        out_specs=[vmem] * 8,
        out_shape=[shape(rows, cols)] * 2
        + [shape(packed, cols)] * 2
        + [shape(members, rows, cols), shape(rows, cols), shape(*couplings.shape), shape(rows, cols)],
        scratch_shapes=[pltpu.VMEM((rows, cols), jnp.int32), pltpu.SemaphoreType.DMA((4,))],
        compiler_params=params,
        name="pack",
    )(right_side, center, couplings, land_sea)

    from_west = shifted(east, "lon", 1, True)
    from_east = shifted(west, "lon", -1, True)
    lon_count = lax.axis_size("lon")
    row_start = (lax.axis_size("lat") - 1) * lon_count
    ring = [north]
    for k in range(1, lon_count):
        pairs = [(row_start + i, row_start + (i + k) % lon_count) for i in range(lon_count)]
        ring.append(lax.ppermute(north, ("lat", "lon"), pairs))
    in_west = (lax.broadcasted_iota(jnp.int32, (SUB, cols), 1) % (2 * DEPTH)) < DEPTH
    upper = jnp.where(in_west, from_west[rows - SUB :], from_east[rows - SUB :])
    lower = jnp.where(in_west, from_west[:SUB], from_east[:SUB])
    from_south = shifted(jnp.concatenate([north, upper]), "lat", 1, False)
    from_north = shifted(jnp.concatenate([south, lower]), "lat", -1, False)

    tall = rows + 2 * TOP
    first, second, third, moments = pl.pallas_call(
        stencil_kernel,
        in_specs=[smem] + [vmem] * (8 + lon_count),
        out_specs=[vmem] * 4,
        out_shape=[shape(members, rows, cols)] * 3 + [shape(SUB, cols)],
        scratch_shapes=[
            pltpu.VMEM((fields, tall, 2 * cols), f32),
            pltpu.VMEM((8, tall, 2 * cols), f32),
            pltpu.VMEM((members, tall, 2 * cols), f32),
            pltpu.VMEM((members, tall, 2 * cols), f32),
        ],
        compiler_params=params,
        name="stencil",
    )(fold_partner, scaled, weights, edges, scale, from_west, from_east, from_north, from_south, *ring)

    for axis in ("lon", "lat"):
        count = lax.axis_size(axis)
        span = 1
        while span < count:
            radix = 2 if (count // span).bit_length() % 2 == 0 else 4
            parts = [moments]
            for step in range(1, radix):
                parts.append(lax.ppermute(moments, axis, [(i, i ^ (step * span)) for i in range(count)]))
            moments = sum(parts[1:], parts[0])
            span *= radix

    return tuple(
        pl.pallas_call(
            combine_kernel,
            in_specs=[vmem] * 6,
            out_specs=[vmem] * 2,
            out_shape=[shape(members, rows, cols)] * 2,
            compiler_params=params,
            name="combine",
        )(moments, scaled, scale, first, second, third)
    )


def solution(mesh):
    return jax.shard_map(
        body,
        mesh=mesh,
        in_specs=(
            P(None, "lat", "lon"),
            P("lat", "lon"),
            P(None, "lat", "lon"),
            P("lat", "lon"),
            P(),
        ),
        out_specs=(P(None, "lat", "lon"), P(None, "lat", "lon")),
        check_vma=False,
    )
```

```python
import jax
import jax.numpy as jnp
from jax import lax
from jax.experimental import pallas as pl
from jax.experimental.pallas import tpu as pltpu
from jax.sharding import PartitionSpec as P

ITERS = 3
DEPTH = ITERS
SUB = 8
TOP = 2 * SUB


def pack_kernel(
    rhs, center, couplings, land, east, west, north, south, scaled, weights, edges, scale, mask, arrivals
):
    members = rhs.shape[0]
    fields = members + couplings.shape[0] + 1
    rows, cols = center.shape
    lane = lax.broadcasted_iota(jnp.int32, (SUB, cols), 1)
    group = 2 * DEPTH
    pairs = ((land, mask), (center, scale), (rhs, scaled), (couplings, edges))
    copies = [pltpu.make_async_copy(a, b, arrivals.at[i]) for i, (a, b) in enumerate(pairs)]
    for copy in copies:
        copy.start()
    for copy in copies:
        copy.wait()

    def step(index, carry):
        at = pl.multiple_of(index * SUB, SUB)
        here = pl.ds(at, SUB)
        weight = mask[here, :].astype(jnp.float32) / scale[here, :]
        weights[here, :] = weight
        values = []
        for m in range(members):
            value = scaled[m, here, :] * weight
            scaled[m, here, :] = value
            values.append(value)
        values += [edges[c, here, :] for c in range(edges.shape[0])]
        values.append(weight)
        to_east = jnp.zeros((SUB, cols), jnp.float32)
        to_west = jnp.zeros((SUB, cols), jnp.float32)
        for f, value in enumerate(values):
            base = group * f
            moved = pltpu.roll(value, (base + DEPTH) % cols, 1)
            pick_east = jnp.logical_and(lane >= base, lane < base + DEPTH)
            pick_west = jnp.logical_and(lane >= base + DEPTH, lane < base + group)
            to_east = jnp.where(pick_east, moved, to_east)
            to_west = jnp.where(pick_west, moved, to_west)
        east[here, :] = to_east
        west[here, :] = to_west
        return carry

    lax.fori_loop(0, rows // SUB, step, 0, unroll=2)
    copies = north.shape[0]
    for ref, at in ((north.at[0], rows - DEPTH), (south, 0)):
        span = slice(at, at + DEPTH)
        for f in range(fields):
            if f < members:
                value = scaled[f, span, :]
            elif f < fields - 1:
                value = edges[f - members, span, :]
            else:
                value = weights[span, :]
            ref[DEPTH * f : DEPTH * (f + 1), :] = value
        used = DEPTH * fields
        ref[used:, :] = jnp.zeros((ref.shape[0] - used, cols), jnp.float32)
    top = north[0]
    for b in range(1, copies):
        north[b] = top


def stencil_kernel(
    partner, scaled, weights, couplings, center, from_west, from_east, from_north, from_south, ring,
    first, second, third, moments, held, coeff, level_one, level_two,
):
    members = scaled.shape[0]
    edges = couplings.shape[0]
    fields = members + edges + 1
    rows, cols = center.shape
    group = 2 * DEPTH
    wide = 2 * cols
    blocks = ring.shape[0]
    packed = ring.shape[1]
    f_east, f_north, f_ne, f_nw, f_weight = (members + c for c in range(5))
    lat_last = lax.axis_index("lat") == lax.axis_size("lat") - 1
    first_col = lax.axis_index("lon") * cols
    lane = lax.broadcasted_iota(jnp.int32, (SUB, cols), 1)
    in_west = lane % group < DEPTH
    bottom = TOP + rows

    zeros = jnp.zeros((SUB, wide), jnp.float32)
    for at in (0, SUB, bottom, bottom + SUB):
        for f in range(fields):
            held[f, at : at + SUB, :] = zeros
    for at in (0, bottom + SUB):
        for m in range(members):
            level_one[m, at : at + SUB, :] = zeros
            level_two[m, at : at + SUB, :] = zeros

    def spread(value, f):
        return pltpu.roll(value, (cols - group * f - DEPTH) % cols, 1)

    def fill(index, carry):
        at = pl.multiple_of(index * SUB, SUB)
        to = pl.multiple_of(index * SUB + TOP, SUB)
        side = jnp.where(in_west, from_west[pl.ds(at, SUB), :], from_east[pl.ds(at, SUB), :])
        for f in range(fields):
            if f < members:
                value = scaled[f, pl.ds(at, SUB), :]
            elif f < f_weight:
                value = couplings[f - members, pl.ds(at, SUB), :]
            else:
                value = weights[pl.ds(at, SUB), :]
            held[f, pl.ds(to, SUB), :cols] = value
            held[f, pl.ds(to, SUB), cols:] = spread(side, f)
        return carry

    lax.fori_loop(0, rows // SUB, fill, 0)

    side_south = from_south[packed : packed + SUB, :]
    for f in range(fields):
        held[f, TOP - DEPTH : TOP, :cols] = from_south[DEPTH * f : DEPTH * (f + 1), :]
        held[f, TOP - DEPTH : TOP, cols:] = spread(side_south, f)[SUB - DEPTH :, :]

    @pl.when(jnp.logical_not(lat_last))
    def _():
        side_north = from_north[packed : packed + SUB, :]
        for f in range(fields):
            held[f, bottom : bottom + DEPTH, :cols] = from_north[DEPTH * f : DEPTH * (f + 1), :]
            held[f, bottom : bottom + DEPTH, cols:] = spread(side_north, f)[:DEPTH, :]

    @pl.when(lat_last)
    def _():
        total = blocks * cols
        shift = cols.bit_length() - 1
        row = lax.broadcasted_iota(jnp.int32, (packed, cols), 0)
        spot = lax.broadcasted_iota(jnp.int32, (packed, cols), 1)

        def of(f):
            return jnp.logical_and(row >= DEPTH * f, row < DEPTH * (f + 1))

        offset = jnp.where(jnp.logical_or(of(f_east), of(f_ne)), -1, jnp.where(of(f_nw), 1, 0))
        beside = jnp.where(spot < cols // 2, spot + cols, spot - cols)
        mirrored = []
        for column in (spot, beside):
            source = partner[0] - first_col + offset - column
            source = jnp.where(source < 0, source + total, source)
            source = jnp.where(source < 0, source + total, source)
            source = jnp.where(source >= total, source - total, source)
            block = lax.shift_right_logical(source, shift)
            place = jnp.bitwise_and(source, cols - 1)
            found = jnp.zeros((packed, cols), jnp.float32)
            for b in range(blocks):
                taken = jnp.take_along_axis(ring[b], place, axis=1, mode="promise_in_bounds")
                found = jnp.where(block == b, taken, found)
            mirrored.append(found)
        for half, found in enumerate(mirrored):
            lanes = slice(half * cols, (half + 1) * cols)
            for f in range(fields):
                back = 2 if f in (f_north, f_ne, f_nw) else 1
                for k in range(DEPTH):
                    at = DEPTH - back - k
                    if at >= 0:
                        spot_row = DEPTH * f + at
                        held[f, bottom + k : bottom + k + 1, lanes] = found[spot_row : spot_row + 1, :]
            top = slice(bottom - 1, bottom)
            across = found[DEPTH * f_north + DEPTH - 1 : DEPTH * (f_north + 1), :]
            held[f_north, top, lanes] = 0.5 * (held[f_north, top, lanes] + across)
            held[f_ne, top, lanes] = jnp.zeros((1, cols), jnp.float32)
            held[f_nw, top, lanes] = jnp.zeros((1, cols), jnp.float32)

    def east_of(value):
        return pltpu.roll(value, wide - 1, 1)

    def west_of(value):
        return pltpu.roll(value, 1, 1)

    def around(ref, at):
        return ref.at[:, pl.ds(pl.multiple_of(at - SUB, SUB), 3 * SUB), :]

    def make_coeff(index, carry):
        at = pl.multiple_of(index * SUB, SUB)
        here = pl.ds(at, SUB)
        near = around(held, at)
        weight = held[f_weight, here, :]
        weight_east = east_of(weight)
        weight_west = west_of(weight)
        coeff[0, here, :] = west_of(weight * held[f_east, here, :])
        coeff[1, here, :] = west_of(weight * held[f_ne, here, :])
        coeff[2, here, :] = weight_west * near[f_nw, SUB - 1 : 2 * SUB - 1, :]
        coeff[3, here, :] = weight_east * held[f_east, here, :]
        coeff[4, here, :] = east_of(weight * held[f_nw, here, :])
        coeff[5, here, :] = weight_east * near[f_ne, SUB - 1 : 2 * SUB - 1, :]
        coeff[6, here, :] = weight * held[f_north, here, :]
        coeff[7, here, :] = weight * near[f_north, SUB - 1 : 2 * SUB - 1, :]
        return carry

    wide_row = lax.broadcasted_iota(jnp.int32, (SUB, wide), 0)
    is_first = wide_row == 0
    is_last = wide_row == SUB - 1
    chunks = rows // SUB
    lax.fori_loop(1, chunks + 3, make_coeff, 0)

    def level(source, target, result):
        def chunk(index, carry, inside):
            at = pl.multiple_of(index * SUB, SUB)
            here = pl.ds(at, SUB)
            c = [coeff[k, here, :] for k in range(8)]
            if inside:
                inner = pl.ds(pl.multiple_of(at - TOP, SUB), SUB)
                scale = center[inner, :]
            sums = []
            after = pl.ds(pl.multiple_of(at + SUB, SUB), SUB)
            before = pl.ds(pl.multiple_of(at - SUB, SUB), SUB)
            for m in range(members):
                mid = source[m, here, :]
                up = pltpu.roll(jnp.where(is_first, source[m, after, :], mid), SUB - 1, 0)
                down = pltpu.roll(jnp.where(is_last, source[m, before, :], mid), 1, 0)
                new = c[6] * up + c[7] * down
                new = new + east_of(c[0] * mid + c[1] * up + c[2] * down)
                new = new + west_of(c[3] * mid + c[4] * up + c[5] * down)
                if target is not None:
                    target[m, here, :] = new
                if inside:
                    kept = new[:, :cols]
                    result[m, inner, :] = kept
                    scaled = scale * mid[:, :cols]
                    sums.append(carry[2 * m] + scaled * mid[:, :cols])
                    sums.append(carry[2 * m + 1] + scaled * kept)
            return tuple(sums) if inside else carry

        start = tuple(jnp.zeros((SUB, cols), jnp.float32) for _ in range(2 * members))
        if target is not None:
            chunk(1, 0, False)
        out = lax.fori_loop(2, chunks + 2, lambda i, s: chunk(i, s, True), start)
        if target is not None:
            chunk(chunks + 2, 0, False)
        return out

    totals = [level(held, level_one, first), level(level_one, level_two, second), level(level_two, None, third)]
    out_row = lax.broadcasted_iota(jnp.int32, (SUB, cols), 0)
    tile = jnp.zeros((SUB, cols), jnp.float32)
    for k in range(2 * DEPTH):
        gathered = jnp.zeros((SUB, cols), jnp.float32)
        for m in range(members):
            one = jnp.sum(totals[k // 2][2 * m + k % 2], axis=0, keepdims=True)
            gathered = jnp.where(out_row == m, one, gathered)
        tile = jnp.where(lane == k, jnp.sum(gathered, axis=1, keepdims=True), tile)
    for b in range(moments.shape[0]):
        moments[b] = tile


def combine_kernel(moments, zeroth, center, first, second, third, solution, residual):
    def inner(p, q):
        total = 0.0
        for i, a in enumerate(p):
            for j, b in enumerate(q):
                total = total + a * b * nu[i + j]
        return total

    parts = [moments[b] for b in range(moments.shape[0])]
    while len(parts) > 1:
        half = len(parts) // 2
        parts = [a + b for a, b in zip(parts[:half], parts[half : 2 * half])] + parts[2 * half :]
    summed = parts[0]
    nu = [summed[:, k : k + 1] for k in range(2 * DEPTH)]
    one = jnp.ones_like(nu[0])
    scaled = [one]
    direction = [one]
    answer = [jnp.zeros_like(one)] * DEPTH
    gamma = nu[0]
    for iteration in range(DEPTH):
        image = [d - e for d, e in zip(direction + [0.0], [0.0] + direction)]
        step = gamma / inner(direction, image)
        for i, d in enumerate(direction):
            answer[i] = answer[i] + step * d
        scaled = [z - step * q for z, q in zip(scaled + [0.0], image)]
        if iteration + 1 < DEPTH:
            gamma_next = inner(scaled, scaled)
            ratio = gamma_next / gamma
            direction = [z + ratio * d for z, d in zip(scaled, direction + [0.0])]
            gamma = gamma_next

    rows, cols = center.shape
    members = zeroth.shape[0]
    wide_answer = [jnp.broadcast_to(a, (members, cols)) for a in answer]
    wide_scaled = [jnp.broadcast_to(a, (members, cols)) for a in scaled]

    def chunk(index, carry):
        here = pl.ds(pl.multiple_of(index * SUB, SUB), SUB)
        scale = center[here, :]
        for m in range(members):
            basis = [zeroth[m, here, :], first[m, here, :], second[m, here, :], third[m, here, :]]
            got = sum(a[m : m + 1, :] * v for a, v in zip(wide_answer, basis))
            left = sum(a[m : m + 1, :] * v for a, v in zip(wide_scaled, basis))
            solution[m, here, :] = got
            residual[m, here, :] = scale * left
        return carry

    lax.fori_loop(0, rows // SUB, chunk, 0)


def shifted(value, axis, by, closed):
    count = lax.axis_size(axis)
    pairs = [(i, (i + by) % count) for i in range(count) if closed or 0 <= i + by < count]
    return lax.ppermute(value, axis, pairs)


def body(right_side, center, couplings, land_sea, fold_partner):
    members, rows, cols = right_side.shape
    fields = members + couplings.shape[0] + 1
    packed = -(-DEPTH * fields // SUB) * SUB
    f32 = jnp.float32
    vmem = pl.BlockSpec(memory_space=pltpu.VMEM)
    smem = pl.BlockSpec(memory_space=pltpu.SMEM)
    params = pltpu.CompilerParams(vmem_limit_bytes=32 * 1024 * 1024)

    def shape(*dims):
        return jax.ShapeDtypeStruct(dims, f32)

    lon_count = lax.axis_size("lon")
    devices = lon_count * lax.axis_size("lat")
    east, west, north, south, scaled, weights, edges, scale = pl.pallas_call(
        pack_kernel,
        in_specs=[pl.BlockSpec(memory_space=pltpu.HBM)] * 4,
        out_specs=[vmem] * 8,
        out_shape=[shape(rows, cols)] * 2
        + [shape(lon_count, packed, cols), shape(packed, cols)]
        + [shape(members, rows, cols), shape(rows, cols), shape(*couplings.shape), shape(rows, cols)],
        scratch_shapes=[pltpu.VMEM((rows, cols), jnp.int32), pltpu.SemaphoreType.DMA((4,))],
        compiler_params=params,
        name="pack",
    )(right_side, center, couplings, land_sea)

    from_west = shifted(east, "lon", 1, True)
    from_east = shifted(west, "lon", -1, True)
    ring = lax.all_to_all(north, "lon", 0, 0, tiled=False)
    north = north[0]
    in_west = (lax.broadcasted_iota(jnp.int32, (SUB, cols), 1) % (2 * DEPTH)) < DEPTH
    upper = jnp.where(in_west, from_west[rows - SUB :], from_east[rows - SUB :])
    lower = jnp.where(in_west, from_west[:SUB], from_east[:SUB])
    from_south = shifted(jnp.concatenate([north, upper]), "lat", 1, False)
    from_north = shifted(jnp.concatenate([south, lower]), "lat", -1, False)

    tall = rows + 2 * TOP
    first, second, third, moments = pl.pallas_call(
        stencil_kernel,
        in_specs=[smem] + [vmem] * 9,
        out_specs=[vmem] * 4,
        out_shape=[shape(members, rows, cols)] * 3 + [shape(devices, SUB, cols)],
        scratch_shapes=[
            pltpu.VMEM((fields, tall, 2 * cols), f32),
            pltpu.VMEM((8, tall, 2 * cols), f32),
            pltpu.VMEM((members, tall, 2 * cols), f32),
            pltpu.VMEM((members, tall, 2 * cols), f32),
        ],
        compiler_params=params,
        name="stencil",
    )(fold_partner, scaled, weights, edges, scale, from_west, from_east, from_north, from_south, ring)

    moments = lax.all_to_all(moments, ("lat", "lon"), 0, 0, tiled=False)

    return tuple(
        pl.pallas_call(
            combine_kernel,
            in_specs=[vmem] * 6,
            out_specs=[vmem] * 2,
            out_shape=[shape(members, rows, cols)] * 2,
            compiler_params=params,
            name="combine",
        )(moments, scaled, scale, first, second, third)
    )


def solution(mesh):
    return jax.shard_map(
        body,
        mesh=mesh,
        in_specs=(
            P(None, "lat", "lon"),
            P("lat", "lon"),
            P(None, "lat", "lon"),
            P("lat", "lon"),
            P(),
        ),
        out_specs=(P(None, "lat", "lon"), P(None, "lat", "lon")),
        check_vma=False,
    )
```

```python
import jax
import jax.numpy as jnp
from jax import lax
from jax.experimental import pallas as pl
from jax.experimental.pallas import tpu as pltpu
from jax.sharding import PartitionSpec as P

ITERS = 3
DEPTH = ITERS
SUB = 8
TOP = 2 * SUB


def pack_kernel(
    rhs, center, couplings, land, east, west, spread_north, north, south, scaled, weights, edges, scale, mask, arrivals
):
    members = rhs.shape[0]
    fields = members + couplings.shape[0] + 1
    rows, cols = center.shape
    lane = lax.broadcasted_iota(jnp.int32, (SUB, cols), 1)
    group = 2 * DEPTH
    pairs = ((land, mask), (center, scale), (rhs, scaled), (couplings, edges))
    copies = [pltpu.make_async_copy(a, b, arrivals.at[i]) for i, (a, b) in enumerate(pairs)]
    for copy in copies:
        copy.start()
    for copy in copies:
        copy.wait()

    def step(index, carry):
        at = pl.multiple_of(index * SUB, SUB)
        here = pl.ds(at, SUB)
        weight = mask[here, :].astype(jnp.float32) / scale[here, :]
        weights[here, :] = weight
        values = []
        for m in range(members):
            value = scaled[m, here, :] * weight
            scaled[m, here, :] = value
            values.append(value)
        values += [edges[c, here, :] for c in range(edges.shape[0])]
        values.append(weight)
        to_east = jnp.zeros((SUB, cols), jnp.float32)
        to_west = jnp.zeros((SUB, cols), jnp.float32)
        for f, value in enumerate(values):
            base = group * f
            moved = pltpu.roll(value, (base + DEPTH) % cols, 1)
            pick_east = jnp.logical_and(lane >= base, lane < base + DEPTH)
            pick_west = jnp.logical_and(lane >= base + DEPTH, lane < base + group)
            to_east = jnp.where(pick_east, moved, to_east)
            to_west = jnp.where(pick_west, moved, to_west)
        east[here, :] = to_east
        west[here, :] = to_west
        return carry

    lax.fori_loop(0, rows // SUB, step, 0, unroll=2)
    for ref, at in ((north, rows - DEPTH), (south, 0)):
        span = slice(at, at + DEPTH)
        for f in range(fields):
            if f < members:
                value = scaled[f, span, :]
            elif f < fields - 1:
                value = edges[f - members, span, :]
            else:
                value = weights[span, :]
            ref[DEPTH * f : DEPTH * (f + 1), :] = value
        used = DEPTH * fields
        ref[used:, :] = jnp.zeros((ref.shape[0] - used, cols), jnp.float32)
    top = north[...]
    for b in range(spread_north.shape[0]):
        spread_north[b] = top


def stencil_kernel(
    partner, scaled, weights, couplings, center, from_west, from_east, from_north, from_south, ring,
    first, second, third, moments, held, coeff, level_one, level_two,
):
    members = scaled.shape[0]
    edges = couplings.shape[0]
    fields = members + edges + 1
    rows, cols = center.shape
    group = 2 * DEPTH
    wide = 2 * cols
    blocks = ring.shape[0]
    packed = ring.shape[1]
    f_east, f_north, f_ne, f_nw, f_weight = (members + c for c in range(5))
    lat_last = lax.axis_index("lat") == lax.axis_size("lat") - 1
    first_col = lax.axis_index("lon") * cols
    lane = lax.broadcasted_iota(jnp.int32, (SUB, cols), 1)
    in_west = lane % group < DEPTH
    bottom = TOP + rows

    zeros = jnp.zeros((SUB, wide), jnp.float32)
    for at in (0, SUB, bottom, bottom + SUB):
        for f in range(fields):
            held[f, at : at + SUB, :] = zeros
    for at in (0, bottom + SUB):
        for m in range(members):
            level_one[m, at : at + SUB, :] = zeros
            level_two[m, at : at + SUB, :] = zeros

    def spread(value, f):
        return pltpu.roll(value, (cols - group * f - DEPTH) % cols, 1)

    def fill(index, carry):
        at = pl.multiple_of(index * SUB, SUB)
        to = pl.multiple_of(index * SUB + TOP, SUB)
        side = jnp.where(in_west, from_west[pl.ds(at, SUB), :], from_east[pl.ds(at, SUB), :])
        for f in range(fields):
            if f < members:
                value = scaled[f, pl.ds(at, SUB), :]
            elif f < f_weight:
                value = couplings[f - members, pl.ds(at, SUB), :]
            else:
                value = weights[pl.ds(at, SUB), :]
            held[f, pl.ds(to, SUB), :cols] = value
            held[f, pl.ds(to, SUB), cols:] = spread(side, f)
        return carry

    lax.fori_loop(0, rows // SUB, fill, 0)

    side_south = from_south[packed : packed + SUB, :]
    for f in range(fields):
        held[f, TOP - DEPTH : TOP, :cols] = from_south[DEPTH * f : DEPTH * (f + 1), :]
        held[f, TOP - DEPTH : TOP, cols:] = spread(side_south, f)[SUB - DEPTH :, :]

    @pl.when(jnp.logical_not(lat_last))
    def _():
        side_north = from_north[packed : packed + SUB, :]
        for f in range(fields):
            held[f, bottom : bottom + DEPTH, :cols] = from_north[DEPTH * f : DEPTH * (f + 1), :]
            held[f, bottom : bottom + DEPTH, cols:] = spread(side_north, f)[:DEPTH, :]

    @pl.when(lat_last)
    def _():
        total = blocks * cols
        shift = cols.bit_length() - 1
        row = lax.broadcasted_iota(jnp.int32, (packed, cols), 0)
        spot = lax.broadcasted_iota(jnp.int32, (packed, cols), 1)

        def of(f):
            return jnp.logical_and(row >= DEPTH * f, row < DEPTH * (f + 1))

        offset = jnp.where(jnp.logical_or(of(f_east), of(f_ne)), -1, jnp.where(of(f_nw), 1, 0))
        beside = jnp.where(spot < cols // 2, spot + cols, spot - cols)
        mirrored = []
        for column in (spot, beside):
            source = partner[0] - first_col + offset - column
            source = jnp.where(source < 0, source + total, source)
            source = jnp.where(source < 0, source + total, source)
            source = jnp.where(source >= total, source - total, source)
            block = lax.shift_right_logical(source, shift)
            place = jnp.bitwise_and(source, cols - 1)
            found = jnp.zeros((packed, cols), jnp.float32)
            for b in range(blocks):
                taken = jnp.take_along_axis(ring[b], place, axis=1, mode="promise_in_bounds")
                found = jnp.where(block == b, taken, found)
            mirrored.append(found)
        for half, found in enumerate(mirrored):
            lanes = slice(half * cols, (half + 1) * cols)
            for f in range(fields):
                back = 2 if f in (f_north, f_ne, f_nw) else 1
                for k in range(DEPTH):
                    at = DEPTH - back - k
                    if at >= 0:
                        spot_row = DEPTH * f + at
                        held[f, bottom + k : bottom + k + 1, lanes] = found[spot_row : spot_row + 1, :]
            top = slice(bottom - 1, bottom)
            across = found[DEPTH * f_north + DEPTH - 1 : DEPTH * (f_north + 1), :]
            held[f_north, top, lanes] = 0.5 * (held[f_north, top, lanes] + across)
            held[f_ne, top, lanes] = jnp.zeros((1, cols), jnp.float32)
            held[f_nw, top, lanes] = jnp.zeros((1, cols), jnp.float32)

    def east_of(value):
        return pltpu.roll(value, wide - 1, 1)

    def west_of(value):
        return pltpu.roll(value, 1, 1)

    def around(ref, at):
        return ref.at[:, pl.ds(pl.multiple_of(at - SUB, SUB), 3 * SUB), :]

    def make_coeff(index, carry):
        at = pl.multiple_of(index * SUB, SUB)
        here = pl.ds(at, SUB)
        near = around(held, at)
        weight = held[f_weight, here, :]
        weight_east = east_of(weight)
        weight_west = west_of(weight)
        coeff[0, here, :] = west_of(weight * held[f_east, here, :])
        coeff[1, here, :] = west_of(weight * held[f_ne, here, :])
        coeff[2, here, :] = weight_west * near[f_nw, SUB - 1 : 2 * SUB - 1, :]
        coeff[3, here, :] = weight_east * held[f_east, here, :]
        coeff[4, here, :] = east_of(weight * held[f_nw, here, :])
        coeff[5, here, :] = weight_east * near[f_ne, SUB - 1 : 2 * SUB - 1, :]
        coeff[6, here, :] = weight * held[f_north, here, :]
        coeff[7, here, :] = weight * near[f_north, SUB - 1 : 2 * SUB - 1, :]
        return carry

    wide_row = lax.broadcasted_iota(jnp.int32, (SUB, wide), 0)
    is_first = wide_row == 0
    is_last = wide_row == SUB - 1
    chunks = rows // SUB
    lax.fori_loop(1, chunks + 3, make_coeff, 0)

    def level(source, target, result):
        def chunk(index, carry, inside):
            at = pl.multiple_of(index * SUB, SUB)
            here = pl.ds(at, SUB)
            c = [coeff[k, here, :] for k in range(8)]
            if inside:
                inner = pl.ds(pl.multiple_of(at - TOP, SUB), SUB)
                scale = center[inner, :]
            sums = []
            after = pl.ds(pl.multiple_of(at + SUB, SUB), SUB)
            before = pl.ds(pl.multiple_of(at - SUB, SUB), SUB)
            for m in range(members):
                mid = source[m, here, :]
                up = pltpu.roll(jnp.where(is_first, source[m, after, :], mid), SUB - 1, 0)
                down = pltpu.roll(jnp.where(is_last, source[m, before, :], mid), 1, 0)
                new = c[6] * up + c[7] * down
                new = new + east_of(c[0] * mid + c[1] * up + c[2] * down)
                new = new + west_of(c[3] * mid + c[4] * up + c[5] * down)
                if target is not None:
                    target[m, here, :] = new
                if inside:
                    kept = new[:, :cols]
                    result[m, inner, :] = kept
                    scaled = scale * mid[:, :cols]
                    sums.append(carry[2 * m] + scaled * mid[:, :cols])
                    sums.append(carry[2 * m + 1] + scaled * kept)
            return tuple(sums) if inside else carry

        start = tuple(jnp.zeros((SUB, cols), jnp.float32) for _ in range(2 * members))
        if target is not None:
            chunk(1, 0, False)
        out = lax.fori_loop(2, chunks + 2, lambda i, s: chunk(i, s, True), start)
        if target is not None:
            chunk(chunks + 2, 0, False)
        return out

    totals = [level(held, level_one, first), level(level_one, level_two, second), level(level_two, None, third)]
    out_row = lax.broadcasted_iota(jnp.int32, (SUB, cols), 0)
    tile = jnp.zeros((SUB, cols), jnp.float32)
    for k in range(2 * DEPTH):
        gathered = jnp.zeros((SUB, cols), jnp.float32)
        for m in range(members):
            one = jnp.sum(totals[k // 2][2 * m + k % 2], axis=0, keepdims=True)
            gathered = jnp.where(out_row == m, one, gathered)
        tile = jnp.where(lane == k, jnp.sum(gathered, axis=1, keepdims=True), tile)
    for b in range(moments.shape[0]):
        moments[b] = tile


def combine_kernel(moments, zeroth, center, first, second, third, solution, residual, got, left, sent):
    def inner(p, q):
        total = 0.0
        for i, a in enumerate(p):
            for j, b in enumerate(q):
                total = total + a * b * nu[i + j]
        return total

    parts = [moments[b] for b in range(moments.shape[0])]
    while len(parts) > 1:
        half = len(parts) // 2
        parts = [a + b for a, b in zip(parts[:half], parts[half : 2 * half])] + parts[2 * half :]
    summed = parts[0]
    nu = [summed[:, k : k + 1] for k in range(2 * DEPTH)]
    one = jnp.ones_like(nu[0])
    scaled = [one]
    direction = [one]
    answer = [jnp.zeros_like(one)] * DEPTH
    gamma = nu[0]
    for iteration in range(DEPTH):
        image = [d - e for d, e in zip(direction + [0.0], [0.0] + direction)]
        step = gamma / inner(direction, image)
        for i, d in enumerate(direction):
            answer[i] = answer[i] + step * d
        scaled = [z - step * q for z, q in zip(scaled + [0.0], image)]
        if iteration + 1 < DEPTH:
            gamma_next = inner(scaled, scaled)
            ratio = gamma_next / gamma
            direction = [z + ratio * d for z, d in zip(scaled, direction + [0.0])]
            gamma = gamma_next

    rows, cols = center.shape
    members = zeroth.shape[0]
    wide_answer = [jnp.broadcast_to(a, (members, cols)) for a in answer]
    wide_scaled = [jnp.broadcast_to(a, (members, cols)) for a in scaled]

    copies = []
    for m in range(members):

        def chunk(index, carry):
            here = pl.ds(pl.multiple_of(index * SUB, SUB), SUB)
            basis = [zeroth[m, here, :], first[m, here, :], second[m, here, :], third[m, here, :]]
            got[m, here, :] = sum(a[m : m + 1, :] * v for a, v in zip(wide_answer, basis))
            left[m, here, :] = center[here, :] * sum(a[m : m + 1, :] * v for a, v in zip(wide_scaled, basis))
            return carry

        lax.fori_loop(0, rows // SUB, chunk, 0, unroll=4)
        for i, (kept, out) in enumerate(((got, solution), (left, residual))):
            copy = pltpu.make_async_copy(kept.at[m], out.at[m], sent.at[i, m])
            copy.start()
            copies.append(copy)
    for copy in copies:
        copy.wait()


def shifted(value, axis, by, closed):
    count = lax.axis_size(axis)
    pairs = [(i, (i + by) % count) for i in range(count) if closed or 0 <= i + by < count]
    return lax.ppermute(value, axis, pairs)


def body(right_side, center, couplings, land_sea, fold_partner):
    members, rows, cols = right_side.shape
    fields = members + couplings.shape[0] + 1
    packed = -(-DEPTH * fields // SUB) * SUB
    f32 = jnp.float32
    vmem = pl.BlockSpec(memory_space=pltpu.VMEM)
    smem = pl.BlockSpec(memory_space=pltpu.SMEM)
    params = pltpu.CompilerParams(vmem_limit_bytes=32 * 1024 * 1024)

    def shape(*dims):
        return jax.ShapeDtypeStruct(dims, f32)

    lon_count = lax.axis_size("lon")
    devices = lon_count * lax.axis_size("lat")
    east, west, spread_north, north, south, scaled, weights, edges, scale = pl.pallas_call(
        pack_kernel,
        in_specs=[pl.BlockSpec(memory_space=pltpu.HBM)] * 4,
        out_specs=[vmem] * 9,
        out_shape=[shape(rows, cols)] * 2
        + [shape(lon_count, packed, cols), shape(packed, cols), shape(packed, cols)]
        + [shape(members, rows, cols), shape(rows, cols), shape(*couplings.shape), shape(rows, cols)],
        scratch_shapes=[pltpu.VMEM((rows, cols), jnp.int32), pltpu.SemaphoreType.DMA((4,))],
        compiler_params=params,
        name="pack",
    )(*(pltpu.with_memory_space_constraint(x, pltpu.HBM) for x in (right_side, center, couplings, land_sea)))

    from_west = shifted(east, "lon", 1, True)
    from_east = shifted(west, "lon", -1, True)
    ring = lax.all_to_all(spread_north, "lon", 0, 0, tiled=False)
    in_west = (lax.broadcasted_iota(jnp.int32, (SUB, cols), 1) % (2 * DEPTH)) < DEPTH
    upper = jnp.where(in_west, from_west[rows - SUB :], from_east[rows - SUB :])
    lower = jnp.where(in_west, from_west[:SUB], from_east[:SUB])
    from_south = shifted(jnp.concatenate([north, upper]), "lat", 1, False)
    from_north = shifted(jnp.concatenate([south, lower]), "lat", -1, False)

    tall = rows + 2 * TOP
    first, second, third, moments = pl.pallas_call(
        stencil_kernel,
        in_specs=[smem] + [vmem] * 9,
        out_specs=[vmem] * 4,
        out_shape=[shape(members, rows, cols)] * 3 + [shape(devices, SUB, cols)],
        scratch_shapes=[
            pltpu.VMEM((fields, tall, 2 * cols), f32),
            pltpu.VMEM((8, tall, 2 * cols), f32),
            pltpu.VMEM((members, tall, 2 * cols), f32),
            pltpu.VMEM((members, tall, 2 * cols), f32),
        ],
        compiler_params=params,
        name="stencil",
    )(fold_partner, scaled, weights, edges, scale, from_west, from_east, from_north, from_south, ring)

    moments = lax.all_to_all(moments, ("lat", "lon"), 0, 0, tiled=False)

    return tuple(
        pl.pallas_call(
            combine_kernel,
            in_specs=[vmem] * 6,
            out_specs=[pl.BlockSpec(memory_space=pltpu.HBM)] * 2,
            out_shape=[shape(members, rows, cols)] * 2,
            scratch_shapes=[pltpu.VMEM((members, rows, cols), f32)] * 2 + [pltpu.SemaphoreType.DMA((2, members))],
            compiler_params=params,
            name="combine",
        )(moments, scaled, scale, first, second, third)
    )


def solution(mesh):
    return jax.shard_map(
        body,
        mesh=mesh,
        in_specs=(
            P(None, "lat", "lon"),
            P("lat", "lon"),
            P(None, "lat", "lon"),
            P("lat", "lon"),
            P(),
        ),
        out_specs=(P(None, "lat", "lon"), P(None, "lat", "lon")),
        check_vma=False,
    )
```

```python
import jax
import jax.numpy as jnp
from jax import lax
from jax.experimental import pallas as pl
from jax.experimental.pallas import tpu as pltpu
from jax.sharding import PartitionSpec as P

ITERS = 3
DEPTH = ITERS
SUB = 8
TOP = 2 * SUB


def pack_kernel(
    rhs, center, couplings, land, east, west, spread_north, north, south, scaled, weights, edges, scale, mask, arrivals
):
    members = rhs.shape[0]
    fields = members + couplings.shape[0] + 1
    rows, cols = center.shape
    lane = lax.broadcasted_iota(jnp.int32, (SUB, cols), 1)
    group = 2 * DEPTH
    pairs = ((land, mask), (center, scale), (rhs, scaled), (couplings, edges))
    copies = [pltpu.make_async_copy(a, b, arrivals.at[i]) for i, (a, b) in enumerate(pairs)]
    for copy in copies:
        copy.start()
    for copy in copies:
        copy.wait()

    def step(index, carry):
        at = pl.multiple_of(index * SUB, SUB)
        here = pl.ds(at, SUB)
        weight = mask[here, :].astype(jnp.float32) / scale[here, :]
        weights[here, :] = weight
        values = []
        for m in range(members):
            value = scaled[m, here, :] * weight
            scaled[m, here, :] = value
            values.append(value)
        values += [edges[c, here, :] for c in range(edges.shape[0])]
        values.append(weight)
        to_east = jnp.zeros((SUB, cols), jnp.float32)
        to_west = jnp.zeros((SUB, cols), jnp.float32)
        for f, value in enumerate(values):
            base = group * f
            moved = pltpu.roll(value, (base + DEPTH) % cols, 1)
            pick_east = jnp.logical_and(lane >= base, lane < base + DEPTH)
            pick_west = jnp.logical_and(lane >= base + DEPTH, lane < base + group)
            to_east = jnp.where(pick_east, moved, to_east)
            to_west = jnp.where(pick_west, moved, to_west)
        east[here, :] = to_east
        west[here, :] = to_west
        return carry

    lax.fori_loop(0, rows // SUB, step, 0, unroll=4)
    for ref, at in ((north, rows - DEPTH), (south, 0)):
        span = slice(at, at + DEPTH)
        for f in range(fields):
            if f < members:
                value = scaled[f, span, :]
            elif f < fields - 1:
                value = edges[f - members, span, :]
            else:
                value = weights[span, :]
            ref[DEPTH * f : DEPTH * (f + 1), :] = value
        used = DEPTH * fields
        ref[used:, :] = jnp.zeros((ref.shape[0] - used, cols), jnp.float32)
    top = north[...]
    for b in range(spread_north.shape[0]):
        spread_north[b] = top


def stencil_kernel(
    partner, scaled, weights, couplings, center, from_west, from_east, from_north, from_south, ring,
    first, second, third, moments, held, coeff, level_one, level_two,
):
    members = scaled.shape[0]
    edges = couplings.shape[0]
    fields = members + edges + 1
    rows, cols = center.shape
    group = 2 * DEPTH
    wide = 2 * cols
    blocks = ring.shape[0]
    packed = ring.shape[1]
    f_east, f_north, f_ne, f_nw, f_weight = (members + c for c in range(5))
    lat_last = lax.axis_index("lat") == lax.axis_size("lat") - 1
    first_col = lax.axis_index("lon") * cols
    lane = lax.broadcasted_iota(jnp.int32, (SUB, cols), 1)
    in_west = lane % group < DEPTH
    bottom = TOP + rows

    zeros = jnp.zeros((SUB, wide), jnp.float32)
    for at in (0, SUB, bottom, bottom + SUB):
        for f in range(fields):
            held[f, at : at + SUB, :] = zeros
    for at in (0, bottom + SUB):
        for m in range(members):
            level_one[m, at : at + SUB, :] = zeros
            level_two[m, at : at + SUB, :] = zeros

    def spread(value, f):
        return pltpu.roll(value, (cols - group * f - DEPTH) % cols, 1)

    def fill(index, carry):
        at = pl.multiple_of(index * SUB, SUB)
        to = pl.multiple_of(index * SUB + TOP, SUB)
        side = jnp.where(in_west, from_west[pl.ds(at, SUB), :], from_east[pl.ds(at, SUB), :])
        for f in range(fields):
            if f < members:
                value = scaled[f, pl.ds(at, SUB), :]
            elif f < f_weight:
                value = couplings[f - members, pl.ds(at, SUB), :]
            else:
                value = weights[pl.ds(at, SUB), :]
            held[f, pl.ds(to, SUB), :cols] = value
            held[f, pl.ds(to, SUB), cols:] = spread(side, f)
        return carry

    lax.fori_loop(0, rows // SUB, fill, 0, unroll=4)

    side_south = from_south[packed : packed + SUB, :]
    for f in range(fields):
        held[f, TOP - DEPTH : TOP, :cols] = from_south[DEPTH * f : DEPTH * (f + 1), :]
        held[f, TOP - DEPTH : TOP, cols:] = spread(side_south, f)[SUB - DEPTH :, :]

    @pl.when(jnp.logical_not(lat_last))
    def _():
        side_north = from_north[packed : packed + SUB, :]
        for f in range(fields):
            held[f, bottom : bottom + DEPTH, :cols] = from_north[DEPTH * f : DEPTH * (f + 1), :]
            held[f, bottom : bottom + DEPTH, cols:] = spread(side_north, f)[:DEPTH, :]

    @pl.when(lat_last)
    def _():
        total = blocks * cols
        shift = cols.bit_length() - 1
        row = lax.broadcasted_iota(jnp.int32, (packed, cols), 0)
        spot = lax.broadcasted_iota(jnp.int32, (packed, cols), 1)

        def of(f):
            return jnp.logical_and(row >= DEPTH * f, row < DEPTH * (f + 1))

        offset = jnp.where(jnp.logical_or(of(f_east), of(f_ne)), -1, jnp.where(of(f_nw), 1, 0))
        beside = jnp.where(spot < cols // 2, spot + cols, spot - cols)
        mirrored = []
        for column in (spot, beside):
            source = partner[0] - first_col + offset - column
            source = jnp.where(source < 0, source + total, source)
            source = jnp.where(source < 0, source + total, source)
            source = jnp.where(source >= total, source - total, source)
            block = lax.shift_right_logical(source, shift)
            place = jnp.bitwise_and(source, cols - 1)
            found = jnp.zeros((packed, cols), jnp.float32)
            for b in range(blocks):
                taken = jnp.take_along_axis(ring[b], place, axis=1, mode="promise_in_bounds")
                found = jnp.where(block == b, taken, found)
            mirrored.append(found)
        for half, found in enumerate(mirrored):
            lanes = slice(half * cols, (half + 1) * cols)
            for f in range(fields):
                back = 2 if f in (f_north, f_ne, f_nw) else 1
                for k in range(DEPTH):
                    at = DEPTH - back - k
                    if at >= 0:
                        spot_row = DEPTH * f + at
                        held[f, bottom + k : bottom + k + 1, lanes] = found[spot_row : spot_row + 1, :]
            top = slice(bottom - 1, bottom)
            across = found[DEPTH * f_north + DEPTH - 1 : DEPTH * (f_north + 1), :]
            held[f_north, top, lanes] = 0.5 * (held[f_north, top, lanes] + across)
            held[f_ne, top, lanes] = jnp.zeros((1, cols), jnp.float32)
            held[f_nw, top, lanes] = jnp.zeros((1, cols), jnp.float32)

    def east_of(value):
        return pltpu.roll(value, wide - 1, 1)

    def west_of(value):
        return pltpu.roll(value, 1, 1)

    def around(ref, at):
        return ref.at[:, pl.ds(pl.multiple_of(at - SUB, SUB), 3 * SUB), :]

    def make_coeff(index, carry):
        at = pl.multiple_of(index * SUB, SUB)
        here = pl.ds(at, SUB)
        near = around(held, at)
        weight = held[f_weight, here, :]
        weight_east = east_of(weight)
        weight_west = west_of(weight)
        coeff[0, here, :] = west_of(weight * held[f_east, here, :])
        coeff[1, here, :] = west_of(weight * held[f_ne, here, :])
        coeff[2, here, :] = weight_west * near[f_nw, SUB - 1 : 2 * SUB - 1, :]
        coeff[3, here, :] = weight_east * held[f_east, here, :]
        coeff[4, here, :] = east_of(weight * held[f_nw, here, :])
        coeff[5, here, :] = weight_east * near[f_ne, SUB - 1 : 2 * SUB - 1, :]
        coeff[6, here, :] = weight * held[f_north, here, :]
        coeff[7, here, :] = weight * near[f_north, SUB - 1 : 2 * SUB - 1, :]
        return carry

    wide_row = lax.broadcasted_iota(jnp.int32, (SUB, wide), 0)
    is_first = wide_row == 0
    is_last = wide_row == SUB - 1
    chunks = rows // SUB
    lax.fori_loop(1, chunks + 3, make_coeff, 0, unroll=2)

    def level(source, target, result):
        def chunk(index, carry, inside):
            at = pl.multiple_of(index * SUB, SUB)
            here = pl.ds(at, SUB)
            c = [coeff[k, here, :] for k in range(8)]
            if inside:
                inner = pl.ds(pl.multiple_of(at - TOP, SUB), SUB)
                scale = center[inner, :]
            sums = []
            after = pl.ds(pl.multiple_of(at + SUB, SUB), SUB)
            before = pl.ds(pl.multiple_of(at - SUB, SUB), SUB)
            for m in range(members):
                mid = source[m, here, :]
                up = pltpu.roll(jnp.where(is_first, source[m, after, :], mid), SUB - 1, 0)
                down = pltpu.roll(jnp.where(is_last, source[m, before, :], mid), 1, 0)
                new = c[6] * up + c[7] * down
                new = new + east_of(c[0] * mid + c[1] * up + c[2] * down)
                new = new + west_of(c[3] * mid + c[4] * up + c[5] * down)
                if target is not None:
                    target[m, here, :] = new
                if inside:
                    kept = new[:, :cols]
                    result[m, inner, :] = kept
                    scaled = scale * mid[:, :cols]
                    sums.append(carry[2 * m] + scaled * mid[:, :cols])
                    sums.append(carry[2 * m + 1] + scaled * kept)
            return tuple(sums) if inside else carry

        start = tuple(jnp.zeros((SUB, cols), jnp.float32) for _ in range(2 * members))
        if target is not None:
            chunk(1, 0, False)
        out = lax.fori_loop(2, chunks + 2, lambda i, s: chunk(i, s, True), start)
        if target is not None:
            chunk(chunks + 2, 0, False)
        return out

    totals = [level(held, level_one, first), level(level_one, level_two, second), level(level_two, None, third)]
    out_row = lax.broadcasted_iota(jnp.int32, (SUB, cols), 0)
    tile = jnp.zeros((SUB, cols), jnp.float32)
    for k in range(2 * DEPTH):
        gathered = jnp.zeros((SUB, cols), jnp.float32)
        for m in range(members):
            one = jnp.sum(totals[k // 2][2 * m + k % 2], axis=0, keepdims=True)
            gathered = jnp.where(out_row == m, one, gathered)
        tile = jnp.where(lane == k, jnp.sum(gathered, axis=1, keepdims=True), tile)
    for b in range(moments.shape[0]):
        moments[b] = tile


def combine_kernel(moments, zeroth, center, first, second, third, solution, residual, got, left, sent):
    def inner(p, q):
        total = 0.0
        for i, a in enumerate(p):
            for j, b in enumerate(q):
                total = total + a * b * nu[i + j]
        return total

    parts = [moments[b] for b in range(moments.shape[0])]
    while len(parts) > 1:
        half = len(parts) // 2
        parts = [a + b for a, b in zip(parts[:half], parts[half : 2 * half])] + parts[2 * half :]
    summed = parts[0]
    nu = [summed[:, k : k + 1] for k in range(2 * DEPTH)]
    one = jnp.ones_like(nu[0])
    scaled = [one]
    direction = [one]
    answer = [jnp.zeros_like(one)] * DEPTH
    gamma = nu[0]
    for iteration in range(DEPTH):
        image = [d - e for d, e in zip(direction + [0.0], [0.0] + direction)]
        step = gamma / inner(direction, image)
        for i, d in enumerate(direction):
            answer[i] = answer[i] + step * d
        scaled = [z - step * q for z, q in zip(scaled + [0.0], image)]
        if iteration + 1 < DEPTH:
            gamma_next = inner(scaled, scaled)
            ratio = gamma_next / gamma
            direction = [z + ratio * d for z, d in zip(scaled, direction + [0.0])]
            gamma = gamma_next

    rows, cols = center.shape
    members = zeroth.shape[0]
    wide_answer = [jnp.broadcast_to(a, (members, cols)) for a in answer]
    wide_scaled = [jnp.broadcast_to(a, (members, cols)) for a in scaled]

    copies = []
    for m in range(members):

        def chunk(index, carry):
            here = pl.ds(pl.multiple_of(index * SUB, SUB), SUB)
            basis = [zeroth[m, here, :], first[m, here, :], second[m, here, :], third[m, here, :]]
            got[m, here, :] = sum(a[m : m + 1, :] * v for a, v in zip(wide_answer, basis))
            left[m, here, :] = center[here, :] * sum(a[m : m + 1, :] * v for a, v in zip(wide_scaled, basis))
            return carry

        lax.fori_loop(0, rows // SUB, chunk, 0, unroll=4)
        for i, (kept, out) in enumerate(((got, solution), (left, residual))):
            copy = pltpu.make_async_copy(kept.at[m], out.at[m], sent.at[i, m])
            copy.start()
            copies.append(copy)
    for copy in copies:
        copy.wait()


def shifted(value, axis, by, closed):
    count = lax.axis_size(axis)
    pairs = [(i, (i + by) % count) for i in range(count) if closed or 0 <= i + by < count]
    return lax.ppermute(value, axis, pairs)


def body(right_side, center, couplings, land_sea, fold_partner):
    members, rows, cols = right_side.shape
    fields = members + couplings.shape[0] + 1
    packed = -(-DEPTH * fields // SUB) * SUB
    f32 = jnp.float32
    vmem = pl.BlockSpec(memory_space=pltpu.VMEM)
    smem = pl.BlockSpec(memory_space=pltpu.SMEM)
    params = pltpu.CompilerParams(vmem_limit_bytes=32 * 1024 * 1024)

    def shape(*dims):
        return jax.ShapeDtypeStruct(dims, f32)

    lon_count = lax.axis_size("lon")
    devices = lon_count * lax.axis_size("lat")
    east, west, spread_north, north, south, scaled, weights, edges, scale = pl.pallas_call(
        pack_kernel,
        in_specs=[pl.BlockSpec(memory_space=pltpu.HBM)] * 4,
        out_specs=[vmem] * 9,
        out_shape=[shape(rows, cols)] * 2
        + [shape(lon_count, packed, cols), shape(packed, cols), shape(packed, cols)]
        + [shape(members, rows, cols), shape(rows, cols), shape(*couplings.shape), shape(rows, cols)],
        scratch_shapes=[pltpu.VMEM((rows, cols), jnp.int32), pltpu.SemaphoreType.DMA((4,))],
        compiler_params=params,
        name="pack",
    )(*(pltpu.with_memory_space_constraint(x, pltpu.HBM) for x in (right_side, center, couplings, land_sea)))

    from_west = shifted(east, "lon", 1, True)
    from_east = shifted(west, "lon", -1, True)
    ring = lax.all_to_all(spread_north, "lon", 0, 0, tiled=False)
    in_west = (lax.broadcasted_iota(jnp.int32, (SUB, cols), 1) % (2 * DEPTH)) < DEPTH
    upper = jnp.where(in_west, from_west[rows - SUB :], from_east[rows - SUB :])
    lower = jnp.where(in_west, from_west[:SUB], from_east[:SUB])
    from_south = shifted(jnp.concatenate([north, upper]), "lat", 1, False)
    from_north = shifted(jnp.concatenate([south, lower]), "lat", -1, False)

    tall = rows + 2 * TOP
    first, second, third, moments = pl.pallas_call(
        stencil_kernel,
        in_specs=[smem] + [vmem] * 9,
        out_specs=[vmem] * 4,
        out_shape=[shape(members, rows, cols)] * 3 + [shape(devices, SUB, cols)],
        scratch_shapes=[
            pltpu.VMEM((fields, tall, 2 * cols), f32),
            pltpu.VMEM((8, tall, 2 * cols), f32),
            pltpu.VMEM((members, tall, 2 * cols), f32),
            pltpu.VMEM((members, tall, 2 * cols), f32),
        ],
        compiler_params=params,
        name="stencil",
    )(fold_partner, scaled, weights, edges, scale, from_west, from_east, from_north, from_south, ring)

    moments = lax.all_to_all(moments, ("lat", "lon"), 0, 0, tiled=False)

    return tuple(
        pl.pallas_call(
            combine_kernel,
            in_specs=[vmem] * 6,
            out_specs=[pl.BlockSpec(memory_space=pltpu.HBM)] * 2,
            out_shape=[shape(members, rows, cols)] * 2,
            scratch_shapes=[pltpu.VMEM((members, rows, cols), f32)] * 2 + [pltpu.SemaphoreType.DMA((2, members))],
            compiler_params=params,
            name="combine",
        )(moments, scaled, scale, first, second, third)
    )


def solution(mesh):
    return jax.shard_map(
        body,
        mesh=mesh,
        in_specs=(
            P(None, "lat", "lon"),
            P("lat", "lon"),
            P(None, "lat", "lon"),
            P("lat", "lon"),
            P(),
        ),
        out_specs=(P(None, "lat", "lon"), P(None, "lat", "lon")),
        check_vma=False,
    )
```
